32 devices in a mesh: seq: 4 (over y, x), fsdp: 8 (over z, core).
Axes of the slice: x: 2, y: 2, z: 4, core: 2. Of those that a mesh axis runs over, the one named last changes fastest.
Arguments:
- token_ids: int32 [8, 1024], P('fsdp', 'seq'), may hold values from 0 to 50303
- segment_ids: int32 [8, 1024], P('fsdp', 'seq'), may hold values from 0 to 7, never falling along the last dimension, each value on 1 to 512 neighbouring positions
- completions: int32 [8, 256], P('fsdp', 'seq'), may hold values from 0 to 1022, as said below
- embedding: float32 [50304, 768], P(None, ('seq', 'fsdp')), may hold values from -1.8 to 1.8
- unembedding: float32 [50304, 768], P('fsdp')
- query_key_value_weight: float32 [2, 768, 2304], P(None, ('seq', 'fsdp')), may hold values from -0.21875 to 0.21875
- attention_output_weight: float32 [2, 768, 768], P(None, ('seq', 'fsdp')), may hold values from -1.75 to 1.75
- up_projection: float32 [2, 768, 3072], P(None, ('seq', 'fsdp')), may hold values from -0.21875 to 0.21875
- down_projection: float32 [2, 3072, 768], P(None, ('seq', 'fsdp')), may hold values from -0.109375 to 0.109375
- vectors: float32 [28, 768], P(None, ('seq', 'fsdp'))
- embedding_mean: float32 [50304, 768], P(None, ('seq', 'fsdp')), may hold values from -4.5776367e-05 to 4.5776367e-05
- unembedding_mean: float32 [50304, 768], P('fsdp'), may hold values from -4.5776367e-05 to 4.5776367e-05
- input_proj_mean: float32 [2, 768, 2304], P(None, ('seq', 'fsdp')), may hold values from -4.5776367e-05 to 4.5776367e-05
- output_proj_mean: float32 [2, 768, 768], P(None, ('seq', 'fsdp')), may hold values from -4.5776367e-05 to 4.5776367e-05
- up_proj_mean: float32 [2, 768, 3072], P(None, ('seq', 'fsdp')), may hold values from -4.5776367e-05 to 4.5776367e-05
- down_proj_mean: float32 [2, 3072, 768], P(None, ('seq', 'fsdp')), may hold values from -4.5776367e-05 to 4.5776367e-05
- vectors_mean: float32 [28, 768], P(None, ('seq', 'fsdp')), may hold values from -4.5776367e-05 to 4.5776367e-05
- embedding_square: float32 [50304, 768], P(None, ('seq', 'fsdp')), may hold values from 1.09382e-11 to 8.75056e-11
- unembedding_square: float32 [50304, 768], P('fsdp'), may hold values from 1.09382e-11 to 8.75056e-11
- input_proj_square: float32 [2, 768, 2304], P(None, ('seq', 'fsdp')), may hold values from 1.09382e-11 to 8.75056e-11
- output_proj_square: float32 [2, 768, 768], P(None, ('seq', 'fsdp')), may hold values from 1.09382e-11 to 8.75056e-11
- up_proj_square: float32 [2, 768, 3072], P(None, ('seq', 'fsdp')), may hold values from 1.09382e-11 to 8.75056e-11
- down_proj_square: float32 [2, 3072, 768], P(None, ('seq', 'fsdp')), may hold values from 1.09382e-11 to 8.75056e-11
- vectors_square: float32 [28, 768], P(None, ('seq', 'fsdp')), may hold values from 1.09382e-11 to 8.75056e-11
Outputs:
- loss: float32 [], replicated
- grad_norm: float32 [], replicated
- embedding_new: float32 [50304, 768], P(None, ('seq', 'fsdp'))
- unembedding_new: float32 [50304, 768], P('fsdp')
- input_proj_new: float32 [2, 768, 2304], P(None, ('seq', 'fsdp'))
- output_proj_new: float32 [2, 768, 768], P(None, ('seq', 'fsdp'))
- up_proj_new: float32 [2, 768, 3072], P(None, ('seq', 'fsdp'))
- down_proj_new: float32 [2, 3072, 768], P(None, ('seq', 'fsdp'))
- vectors_new: float32 [28, 768], P(None, ('seq', 'fsdp'))
- embedding_mean_new: float32 [50304, 768], P(None, ('seq', 'fsdp'))
- unembedding_mean_new: float32 [50304, 768], P('fsdp')
- input_proj_mean_new: float32 [2, 768, 2304], P(None, ('seq', 'fsdp'))
- output_proj_mean_new: float32 [2, 768, 768], P(None, ('seq', 'fsdp'))
- up_proj_mean_new: float32 [2, 768, 3072], P(None, ('seq', 'fsdp'))
- down_proj_mean_new: float32 [2, 3072, 768], P(None, ('seq', 'fsdp'))
- vectors_mean_new: float32 [28, 768], P(None, ('seq', 'fsdp'))
- embedding_square_new: float32 [50304, 768], P(None, ('seq', 'fsdp'))
- unembedding_square_new: float32 [50304, 768], P('fsdp')
- input_proj_square_new: float32 [2, 768, 2304], P(None, ('seq', 'fsdp'))
- output_proj_square_new: float32 [2, 768, 768], P(None, ('seq', 'fsdp'))
- up_proj_square_new: float32 [2, 768, 3072], P(None, ('seq', 'fsdp'))
- down_proj_square_new: float32 [2, 3072, 768], P(None, ('seq', 'fsdp'))
- vectors_square_new: float32 [28, 768], P(None, ('seq', 'fsdp'))
The draws below stay inside these ranges and needn't reach their ends.
Inputs may be any that keep to these rules, and one draw needn't show every extreme that they name: `completions`: within each sequence, entries k * 64 to (k + 1) * 64 - 1 are distinct positions from k * 256 to (k + 1) * 256 - 2.
All inputs are finite; a program needn't handle non-finite values.
Results may differ from the reference program's by a relative error of at most 0.0023.
The reference program's roundings to bfloat16 on the way count: a program that leaves them out, or rounds other values in their place, can miss the bound.
Values may be sent and summed in bfloat16 or wider, within the bound.
A program may use at most 384 MiB of HBM per device.

```python
import math
import jax
import jax.numpy as jnp
import numpy as np
from jax import lax

HEADS = 12
HEAD_DIM = 64
D = 768
FF = 3072
V = 50304
ROT = 16
LAYERS = 2
TOK_DEV = 256
SEQS = 8
LENGTH = 1024
SEL_DEV = 64
NVEC = 28
ADAM_STEP = 3


def draw_completions(key, part):
    blocks = LENGTH // TOK_DEV
    keys = jax.random.split(key, SEQS * blocks)

    def pick(single):
        return jax.random.permutation(single, TOK_DEV - 1)[:SEL_DEV]
    picks = jax.vmap(pick)(keys).reshape(SEQS, blocks, SEL_DEV)
    offsets = (jnp.arange(blocks) * TOK_DEV)[None, :, None]
    return (picks + offsets).reshape(SEQS, blocks * SEL_DEV).astype(jnp.int32)


def common_direction(key):
    return jax.random.normal(jax.random.fold_in(key, 7), (D,), jnp.float32)


def draw_vectors(key, part):
    base = jax.random.normal(jax.random.fold_in(key, 3), (NVEC, D), jnp.float32) * 0.2
    token_rows = jnp.arange(NVEC)
    inner = token_rows % 13
    gain_rows = (token_rows < 13 * LAYERS) & ((inner == 0) | (inner == 2)) | (token_rows == 13 * LAYERS)
    shift_row = jnp.where(token_rows == 13 * LAYERS + 1, 0.5, 0.0)
    return base + jnp.where(gain_rows, 1.0, 0.0)[:, None] + shift_row[:, None] * common_direction(key)[None, :]


def draw_unembedding(key, part):
    base = jax.random.normal(jax.random.fold_in(key, 11), (V, D), jnp.float32) * D ** (-0.5)
    return base + common_direction(key)[None, :] * (4.0 / D)


def plant(drawn, stream_key, smallest, top_value):
    spot = [jax.random.randint(jax.random.fold_in(stream_key, axis), (), 0, length) for axis, length in enumerate(drawn.shape)]
    widest = drawn.shape.index(max(drawn.shape))
    beside = spot[:widest] + [(spot[widest] + 1) % drawn.shape[widest]] + spot[widest + 1:]
    return drawn.at[tuple(spot)].set(smallest).at[tuple(beside)].set(top_value)


def levels(rng, dims, pieces, smallest, largest):
    def one(axis_at, blocks):
        steps = jax.random.uniform(jax.random.fold_in(jax.random.fold_in(rng, 6), axis_at), (blocks,), jnp.float32, smallest / len(pieces), largest / len(pieces))
        return jnp.repeat(jnp.exp(steps), dims[axis_at] // blocks).reshape((-1,) + (1,) * (len(dims) - axis_at - 1))

    factor_of = one(*pieces[0])
    for cut in pieces[1:]:
        factor_of = factor_of * one(*cut)
    return factor_of


def cumulative_ranks(amount, skew):
    loads = [(1 << 20) // math.isqrt(grade ** skew) + 1 for grade in range(1, amount + 1)]
    deviation = 1 + sum(loads) // (1 << 30)
    return np.cumsum(np.array([max(1, weight // deviation) for weight in loads]))


def ranked_ids(stream_key, dims, count, skew):
    table = cumulative_ranks(count, skew)
    ticket = jax.random.randint(jax.random.fold_in(stream_key, 1), dims, 0, int(table[count - 1]))
    rank = jnp.searchsorted(jnp.asarray(table, jnp.int32), ticket, side="right")
    return jax.random.permutation(jax.random.fold_in(stream_key, 2), count)[rank].astype(jnp.int32)


def length_profile(amount, total, most, lean):
    weights = [(1 << 20) // math.isqrt(rank ** lean) + 1 for rank in range(2, amount + 1)]
    rest, counts = total - most - (amount - 1), [1] * (amount - 1)
    while rest > 0:
        movable = [i for i in range(amount - 1) if counts[i] < most]
        pool, remaining = sum([weights[i] for i in movable]), rest
        for i in movable:
            addition = min(most - counts[i], max(1, remaining * weights[i] // pool), rest)
            counts[i] = counts[i] + addition
            rest = rest - addition
    return np.array([most] + counts)


def uneven_parts(own_key, count, total, most, slope):
    if count == 2:
        one = jax.random.randint(own_key, (), max(1, total - most), min(most, total - 1) + 1)
        return jnp.stack([one, total - one])
    tallies = jnp.asarray(length_profile(count, total, most, slope), jnp.int32)
    pairs = (count - 1) // 2
    source_of, taker = tallies[1:1 + 2 * pairs:2], tallies[2:2 + 2 * pairs:2]
    room = jnp.minimum(source_of - 1, most - taker)
    moved = jax.random.randint(jax.random.fold_in(own_key, 1), (pairs,), 0, 1 << 20) % (room + 1)
    tallies = tallies.at[1:1 + 2 * pairs:2].set(source_of - moved).at[2:2 + 2 * pairs:2].set(taker + moved)
    return tallies[jax.random.permutation(jax.random.fold_in(own_key, 2), count)]


def bell_draw(stream_key, dims, scale, limit, pieces=(), dtype=jnp.bfloat16):
    entries = scale * jax.random.normal(stream_key, dims, jnp.float32)
    if pieces:
        entries = entries * levels(stream_key, dims, pieces, -0.22, 0.18)
    return jnp.clip(entries, -limit, limit).astype(dtype)


def setup_inputs(seed: int = 0) -> dict:
    seeds = jax.random.split(jax.random.key(seed), 25)
    return {
        "token_ids": plant(ranked_ids(seeds[0], (SEQS, LENGTH), V, 2), jax.random.fold_in(seeds[0], 3), 0, V - 1).astype(jnp.int32),
        "segment_ids": jax.vmap(lambda own: jnp.searchsorted(jnp.cumsum(uneven_parts(own, 8, LENGTH, LENGTH // 2, 2)), jnp.arange(LENGTH), side="right"))(jax.random.split(seeds[1], SEQS)).reshape((SEQS, LENGTH)).astype(jnp.int32),
        "completions": draw_completions(jax.random.fold_in(seeds[24], 71), 0),
        "embedding": bell_draw(seeds[3], (V, D), 0.3, 1.8, ((1, 32),), jnp.float32),
        "unembedding": draw_unembedding(jax.random.fold_in(seeds[24], 71), 0),
        "query_key_value_weight": bell_draw(seeds[5], (LAYERS, D, 3 * D), D ** -0.5, 0.21875, ((1, 32),), jnp.float32),
        "attention_output_weight": bell_draw(seeds[6], (LAYERS, D, D), (D // 64) ** -0.5, 1.75, ((1, 32),), jnp.float32),
        "up_projection": bell_draw(seeds[7], (LAYERS, D, FF), D ** -0.5, 0.21875, ((1, 32),), jnp.float32),
        "down_projection": bell_draw(seeds[8], (LAYERS, FF, D), FF ** -0.5, 0.109375, ((1, 32),), jnp.float32),
        "vectors": draw_vectors(jax.random.fold_in(seeds[24], 71), 0),
        "embedding_mean": bell_draw(seeds[10], (V, D), (0.028 / ((2 * V * D + LAYERS * (4 * D * D + 2 * D * FF)) ** 0.5)), 4.57763671875e-05, ((1, 32),), jnp.float32),
        "unembedding_mean": bell_draw(seeds[11], (V, D), (0.028 / ((2 * V * D + LAYERS * (4 * D * D + 2 * D * FF)) ** 0.5)), 4.57763671875e-05, ((0, 8),), jnp.float32),
        "input_proj_mean": bell_draw(seeds[12], (LAYERS, D, 3 * D), (0.028 / ((2 * V * D + LAYERS * (4 * D * D + 2 * D * FF)) ** 0.5)), 4.57763671875e-05, ((1, 32),), jnp.float32),
        "output_proj_mean": bell_draw(seeds[13], (LAYERS, D, D), (0.028 / ((2 * V * D + LAYERS * (4 * D * D + 2 * D * FF)) ** 0.5)), 4.57763671875e-05, ((1, 32),), jnp.float32),
        "up_proj_mean": bell_draw(seeds[14], (LAYERS, D, FF), (0.028 / ((2 * V * D + LAYERS * (4 * D * D + 2 * D * FF)) ** 0.5)), 4.57763671875e-05, ((1, 32),), jnp.float32),
        "down_proj_mean": bell_draw(seeds[15], (LAYERS, FF, D), (0.028 / ((2 * V * D + LAYERS * (4 * D * D + 2 * D * FF)) ** 0.5)), 4.57763671875e-05, ((1, 32),), jnp.float32),
        "vectors_mean": bell_draw(seeds[16], (NVEC, D), (0.028 / ((2 * V * D + LAYERS * (4 * D * D + 2 * D * FF)) ** 0.5)), 4.57763671875e-05, ((1, 32),), jnp.float32),
        "embedding_square": jnp.clip(jnp.exp(math.log(8.750559998826901e-11) - 2.0794415 * jax.random.uniform(seeds[17], (V, D), jnp.float32) ** levels(seeds[17], (V, D), ((1, 32),), -0.2, 0.2)), 1.0938199998533626e-11, 8.750559998826901e-11),
        "unembedding_square": jnp.clip(jnp.exp(math.log(8.750559998826901e-11) - 2.0794415 * jax.random.uniform(seeds[18], (V, D), jnp.float32) ** levels(seeds[18], (V, D), ((0, 8),), -0.2, 0.2)), 1.0938199998533626e-11, 8.750559998826901e-11),
        "input_proj_square": jnp.clip(jnp.exp(math.log(8.750559998826901e-11) - 2.0794415 * jax.random.uniform(seeds[19], (LAYERS, D, 3 * D), jnp.float32) ** levels(seeds[19], (LAYERS, D, 3 * D), ((1, 32),), -0.2, 0.2)), 1.0938199998533626e-11, 8.750559998826901e-11),
        "output_proj_square": jnp.clip(jnp.exp(math.log(8.750559998826901e-11) - 2.0794415 * jax.random.uniform(seeds[20], (LAYERS, D, D), jnp.float32) ** levels(seeds[20], (LAYERS, D, D), ((1, 32),), -0.2, 0.2)), 1.0938199998533626e-11, 8.750559998826901e-11),
        "up_proj_square": jnp.clip(jnp.exp(math.log(8.750559998826901e-11) - 2.0794415 * jax.random.uniform(seeds[21], (LAYERS, D, FF), jnp.float32) ** levels(seeds[21], (LAYERS, D, FF), ((1, 32),), -0.2, 0.2)), 1.0938199998533626e-11, 8.750559998826901e-11),
        "down_proj_square": jnp.clip(jnp.exp(math.log(8.750559998826901e-11) - 2.0794415 * jax.random.uniform(seeds[22], (LAYERS, FF, D), jnp.float32) ** levels(seeds[22], (LAYERS, FF, D), ((1, 32),), -0.2, 0.2)), 1.0938199998533626e-11, 8.750559998826901e-11),
        "vectors_square": jnp.clip(jnp.exp(math.log(8.750559998826901e-11) - 2.0794415 * jax.random.uniform(seeds[23], (NVEC, D), jnp.float32) ** levels(seeds[23], (NVEC, D), ((1, 32),), -0.2, 0.2)), 1.0938199998533626e-11, 8.750559998826901e-11),
    }


@jax.custom_vjp
def low(v):
    return lax.optimization_barrier(v.astype(jnp.bfloat16)).astype(jnp.float32)

@jax.custom_vjp
def low_back(v):
    return v

def low_keep(v):
    return (low(v), None)

def low_pass(kept, grad):
    return (grad,)

def back_keep(v):
    return (v, None)

def back_low(kept, grad):
    return (low(grad),)
low.defvjp(low_keep, low_pass)
low_back.defvjp(back_keep, back_low)
highest_precision = lax.Precision.HIGHEST
norm_epsilon = 1e-05
clip_limit = 0.25
learn_rate = 0.03
beta_first = 0.9
beta_second = 0.95
adam_epsilon = 1e-08
decay_weight = 0.1
masked_score = -1000000000.0

def layer_norm(inputs, gain, shift):
    center = inputs - lax.optimization_barrier(jnp.mean(inputs, axis=-1, keepdims=True))
    spread = lax.optimization_barrier(jnp.mean(center * center, axis=-1, keepdims=True))
    return center * lax.rsqrt(spread + norm_epsilon) * gain + shift

def rotate(inputs, places):
    half = ROT // 2
    freq = 1.0 / 10000.0 ** (jnp.arange(half).astype(jnp.float32) * 2.0 / ROT)
    angle = places.astype(jnp.float32)[:, None] * freq[None, :]
    cosine = jnp.cos(angle)[:, None, :]
    sine = jnp.sin(angle)[:, None, :]
    first = inputs[..., :half]
    second = inputs[..., half:ROT]
    return jnp.concatenate([first * cosine - second * sine, second * cosine + first * sine, inputs[..., ROT:]], axis=-1)

def attend_block(rows_q, keyset, valueset, segments, start):
    block = rows_q.shape[0]
    length = keyset.shape[0]
    scale = HEAD_DIM ** (-0.5)
    scores = low_back(jnp.einsum('qhd,khd->hqk', rows_q, keyset, precision=highest_precision) * scale)
    rowpos = start + jnp.arange(block)
    cols = jnp.arange(length)
    rowseg = lax.dynamic_slice_in_dim(segments, start, block, 0)
    allowed = (cols[None, :] <= rowpos[:, None]) & (segments[None, :] == rowseg[:, None])
    scores = jnp.where(allowed[None], scores, masked_score)
    top = lax.optimization_barrier(jnp.max(scores, axis=-1, keepdims=True))
    expo = jnp.exp(scores - top)
    probs = low(expo / lax.optimization_barrier(jnp.sum(expo, axis=-1, keepdims=True)))
    return jnp.einsum('hqk,khd->qhd', probs, valueset, precision=highest_precision)

def attention(queries, keyset, valueset, segments):
    length = queries.shape[1]
    block = min(512, length)
    count = length // block

    def one_seq(items):
        seq_q, seq_k, seq_v, seq_s = items
        shaped = seq_q.reshape(count, block, HEADS, HEAD_DIM)
        starts = jnp.arange(count).astype(jnp.int32) * block
        checked = jax.checkpoint(lambda piece, start: attend_block(piece, seq_k, seq_v, seq_s, start))
        result = lax.map(lambda pair: checked(pair[0], pair[1]), (shaped, starts))
        return result.reshape(length, HEADS, HEAD_DIM)
    return lax.map(one_seq, (queries, keyset, valueset, segments))

def forward(embedding, unembedding, query_key_value_weight, attention_output_weight, up_projection, down_projection, vectors, token_ids, segment_ids, completions):
    seqs, length = token_ids.shape
    table = low(embedding)
    params = low(vectors)
    stream = low_back(jnp.take(table, token_ids, axis=0))
    places = jnp.arange(length)
    for layer_depth in range(LAYERS):
        token_rows = params[13 * layer_depth:13 * layer_depth + 13]
        first_normed = low(layer_norm(stream, token_rows[0], token_rows[1]))
        second_normed = low(layer_norm(stream, token_rows[2], token_rows[3]))
        raw_output = low_back(jnp.einsum('yiu,uw->yiw', first_normed, low(query_key_value_weight[layer_depth]), precision=highest_precision) + token_rows[4:7].reshape(-1))
        split = raw_output.reshape(seqs, length, 3, HEADS, HEAD_DIM)
        queries = low_back(low(rotate(split[:, :, 0], places)))
        keyset = low_back(low(rotate(split[:, :, 1], places)))
        valueset = low_back(low(split[:, :, 2]))
        mixed_output = low_back(low(attention(queries, keyset, valueset, segment_ids)))
        mixed_output = mixed_output.reshape(seqs, length, D)
        attention_branch = low_back(jnp.einsum('yiu,uw->yiw', mixed_output, low(attention_output_weight[layer_depth]), precision=highest_precision) + token_rows[7])
        hidden_state = low_back(jnp.einsum('xvo,on->xvn', second_normed, low(up_projection[layer_depth]), precision=highest_precision) + token_rows[8:12].reshape(-1))
        active_mask = low(jax.nn.gelu(hidden_state, approximate=False))
        feedforward_branch = low_back(jnp.einsum('mak,kp->map', active_mask, low(down_projection[layer_depth]), precision=highest_precision) + token_rows[12])
        stream = stream + attention_branch + feedforward_branch
    final = layer_norm(stream, params[13 * LAYERS], params[13 * LAYERS + 1])
    chosen = low(jax.vmap(lambda rows_f, picks: jnp.take(rows_f, picks, axis=0))(final, completions)).reshape(-1, D)
    targets = jax.vmap(lambda ids_row, picks: jnp.take(ids_row, picks + 1))(token_ids, completions).reshape(-1)
    total_rows = chosen.shape[0]
    block = min(256, total_rows)
    count = total_rows // block
    out_table = low(unembedding)

    def block_loss(items):
        piece, goal = items
        logits = low_back(jnp.dot(piece, out_table.T, precision=highest_precision, preferred_element_type=jnp.float32))
        top = lax.optimization_barrier(jnp.max(logits, axis=-1, keepdims=True))
        logsum = top[:, 0] + jnp.log(lax.optimization_barrier(jnp.sum(jnp.exp(logits - top), axis=-1)))
        hit = jnp.take_along_axis(logits, goal[:, None], axis=1)[:, 0]
        return jnp.sum(logsum - hit)
    parts = lax.map(jax.checkpoint(block_loss), (chosen.reshape(count, block, D), targets.reshape(count, block)))
    return jnp.sum(parts) / total_rows

def adamw(weight, mean, square, grad, factor):
    step = grad * factor
    mean_new = beta_first * mean + (1.0 - beta_first) * step
    square_new = beta_second * square + (1.0 - beta_second) * step * step
    mean_hat = mean_new / (1.0 - beta_first ** ADAM_STEP)
    square_hat = square_new / (1.0 - beta_second ** ADAM_STEP)
    weight_new = weight - learn_rate * (mean_hat / (jnp.sqrt(square_hat) + adam_epsilon) + decay_weight * weight)
    return (weight_new, mean_new, square_new)

def reference(token_ids, segment_ids, completions, embedding, unembedding, query_key_value_weight, attention_output_weight, up_projection, down_projection, vectors, embedding_mean, unembedding_mean, input_proj_mean, output_proj_mean, up_proj_mean, down_proj_mean, vectors_mean, embedding_square, unembedding_square, input_proj_square, output_proj_square, up_proj_square, down_proj_square, vectors_square):
    weights = (embedding, unembedding, query_key_value_weight, attention_output_weight, up_projection, down_projection, vectors)
    loss, pull = jax.vjp(lambda e1, e2, e3, e4, e5, e6, e7: forward(e1, e2, e3, e4, e5, e6, e7, token_ids, segment_ids, completions), *weights)
    grads = pull(jnp.ones((), jnp.float32))
    squares = jnp.zeros((), jnp.float32)
    for grad in grads:
        squares = squares + jnp.sum(grad * grad)
    grad_norm = jnp.sqrt(squares)
    factor = jnp.minimum(1.0, clip_limit / grad_norm)
    means = (embedding_mean, unembedding_mean, input_proj_mean, output_proj_mean, up_proj_mean, down_proj_mean, vectors_mean)
    seconds = (embedding_square, unembedding_square, input_proj_square, output_proj_square, up_proj_square, down_proj_square, vectors_square)
    result = [adamw(weights[index], means[index], seconds[index], grads[index], factor) for index in range(7)]
    return (loss, grad_norm, result[0][0], result[1][0], result[2][0], result[3][0], result[4][0], result[5][0], result[6][0], result[0][1], result[1][1], result[2][1], result[3][1], result[4][1], result[5][1], result[6][1], result[0][2], result[1][2], result[2][2], result[3][2], result[4][2], result[5][2], result[6][2])
```

```python
import functools

import jax
import jax.numpy as jnp
from jax import lax
from jax.experimental import pallas as pl
from jax.experimental.pallas import tpu as pltpu
from jax.sharding import PartitionSpec as P

HEADS = 12
HEAD_DIM = 64
D = 768
ROT = 16
LAYERS = 2
ADAM_STEP = 3

norm_epsilon = 1e-05
clip_limit = 0.25
learn_rate = 0.03
beta_first = 0.9
beta_second = 0.95
adam_epsilon = 1e-08
decay_weight = 0.1
masked_score = -1000000000.0

MESH = pl.DeviceIdType.MESH
BOTH = ("seq", "fsdp")
LOW = jnp.bfloat16


def peer_of(step, axes, sizes):
    here = 0
    count = 1
    for axis, size in zip(axes, sizes):
        here = here * size + lax.axis_index(axis)
        count = count * size
    there = lax.rem(here + step, count)
    coords = {}
    rest = there
    for axis, size in reversed(list(zip(axes, sizes))):
        coords[axis] = lax.rem(rest, size)
        rest = lax.div(rest, size)
    return here, there, coords


def exchange_kernel(axes, sizes, gather, count, *refs):
    arrays = len(gather)
    ins, outs = refs[:arrays], refs[arrays : 2 * arrays]
    send, recv, own = refs[2 * arrays :]
    barrier = pltpu.get_barrier_semaphore()

    def greet(step, carry):
        _, _, coords = peer_of(step, axes, sizes)
        pl.semaphore_signal(barrier, inc=1, device_id=coords, device_id_type=MESH)
        return carry

    lax.fori_loop(1, count, greet, 0)
    pl.semaphore_wait(barrier, count - 1)
    here, _, _ = peer_of(0, axes, sizes)

    def copy(which, step):
        _, there, coords = peer_of(step, axes, sizes)
        source = ins[which] if gather[which] else ins[which].at[there]
        return pltpu.make_async_remote_copy(
            source,
            outs[which].at[here],
            send.at[which, step],
            recv.at[which, step],
            device_id=coords,
            device_id_type=MESH,
        )

    def begin(step, carry):
        for which in range(arrays):
            copy(which, step).start()
        return carry

    def finish(step, carry):
        for which in range(arrays):
            copy(which, step).wait()
        return carry

    lax.fori_loop(1, count, begin, 0)
    locals_ = [
        pltpu.make_async_copy(
            ins[which] if gather[which] else ins[which].at[here],
            outs[which].at[here],
            own.at[which],
        )
        for which in range(arrays)
    ]
    for item in locals_:
        item.start()
    for item in locals_:
        item.wait()
    lax.fori_loop(1, count, finish, 0)


def exchange(values, gather, axes, ident, name):
    sizes = tuple(lax.axis_size(axis) for axis in axes)
    count = 1
    for size in sizes:
        count = count * size
    shapes = [
        jax.ShapeDtypeStruct(((count,) + value.shape) if every else value.shape, value.dtype)
        for value, every in zip(values, gather)
    ]
    arrays = len(values)
    space = pl.BlockSpec(memory_space=pltpu.VMEM)
    return pl.pallas_call(
        functools.partial(exchange_kernel, axes, sizes, tuple(gather), count),
        out_shape=shapes,
        in_specs=[space] * arrays,
        out_specs=[space] * arrays,
        scratch_shapes=[
            pltpu.SemaphoreType.DMA((arrays, count)),
            pltpu.SemaphoreType.DMA((arrays, count)),
            pltpu.SemaphoreType.DMA((arrays,)),
        ],
        compiler_params=pltpu.CompilerParams(collective_id=ident, has_side_effects=True),
        name=name,
    )(*values)


def ring_pairs(size, step):
    return [(place, (place + step) % size) for place in range(size)]


def gather_rows(block, axis):
    size = lax.axis_size(axis)
    here = lax.axis_index(axis)
    out = jnp.zeros((size,) + block.shape, block.dtype)
    out = lax.dynamic_update_index_in_dim(out, block, here, 0)
    for step in range(1, size):
        piece = lax.ppermute(block, axis, ring_pairs(size, step))
        out = lax.dynamic_update_index_in_dim(out, piece, lax.rem(here - step + size, size), 0)
    return out.reshape((size * block.shape[0],) + block.shape[1:])


def scatter_sum(partial, axis):
    size = lax.axis_size(axis)
    here = lax.axis_index(axis)
    blocks = partial.reshape((size, partial.shape[0] // size) + partial.shape[1:])
    pieces = []
    for step in range(1, size):
        piece = lax.dynamic_index_in_dim(blocks, lax.rem(here + step, size), 0, keepdims=False)
        pieces.append(lax.ppermute(piece, axis, ring_pairs(size, step)))
    total = lax.dynamic_index_in_dim(blocks, here, 0, keepdims=False)
    for piece in pieces:
        total = total + piece
    return total


def layer_norm(inputs, gain, shift):
    center = inputs - jnp.mean(inputs, axis=-1, keepdims=True)
    spread = jnp.mean(center * center, axis=-1, keepdims=True)
    return center * lax.rsqrt(spread + norm_epsilon) * gain + shift


def normalized(inputs):
    center = inputs - jnp.mean(inputs, axis=-1, keepdims=True)
    spread = jnp.mean(center * center, axis=-1, keepdims=True)
    scale = lax.rsqrt(spread + norm_epsilon)
    return center * scale, scale


def norm_back(unit, scale, grad_unit):
    first = jnp.mean(grad_unit, axis=-1, keepdims=True)
    second = jnp.mean(grad_unit * unit, axis=-1, keepdims=True)
    return scale * (grad_unit - first - unit * second)


def angles(places):
    half = ROT // 2
    freq = 1.0 / 10000.0 ** (jnp.arange(half).astype(jnp.float32) * 2.0 / ROT)
    angle = places.astype(jnp.float32)[:, None] * freq[None, :]
    return jnp.cos(angle)[:, None, :], jnp.sin(angle)[:, None, :]


def rotate(inputs, cosine, sine):
    half = ROT // 2
    first = inputs[..., :half]
    second = inputs[..., half:ROT]
    return jnp.concatenate(
        [first * cosine - second * sine, second * cosine + first * sine, inputs[..., ROT:]], axis=-1
    )


def rotate_back(inputs, cosine, sine):
    return rotate(inputs, cosine, -sine)


def dot_plain(left, right):
    return jnp.dot(left, right, preferred_element_type=jnp.float32)


def dot_left(left, right):
    return lax.dot_general(
        left, right, (((0,), (0,)), ((), ())), preferred_element_type=jnp.float32
    )


def dot_right(left, right):
    return lax.dot_general(
        left, right, (((1,), (1,)), ((), ())), preferred_element_type=jnp.float32
    )


def seen(rowpos, rowseg, segments):
    cols = jnp.arange(segments.shape[0])
    return (cols[None, :] <= rowpos[:, None]) & (segments[None, :] == rowseg[:, None])


def attend_forward(queries, keyset, valueset, allowed):
    scale = queries.shape[-1] ** (-0.5)
    scores = jnp.einsum("qhd,khd->hqk", queries, keyset, preferred_element_type=jnp.float32) * scale
    scores = jnp.where(allowed[None], scores, masked_score)
    top = jnp.max(scores, axis=-1, keepdims=True)
    expo = jnp.exp(scores - top)
    total = jnp.sum(expo, axis=-1, keepdims=True)
    probs = (expo / total).astype(LOW)
    result = jnp.einsum("hqk,khd->qhd", probs, valueset, preferred_element_type=jnp.float32)
    return result.astype(LOW), (top + jnp.log(total))[..., 0]


def attend_backward(queries, keyset, valueset, allowed, logsum, grad_out):
    scale = queries.shape[-1] ** (-0.5)
    scores = jnp.einsum("qhd,khd->hqk", queries, keyset, preferred_element_type=jnp.float32) * scale
    scores = jnp.where(allowed[None], scores, masked_score)
    probs = jnp.exp(scores - logsum[..., None])
    grad_probs = jnp.einsum("qhd,khd->hqk", grad_out, valueset, preferred_element_type=jnp.float32)
    inner = jnp.sum(probs * grad_probs, axis=-1, keepdims=True)
    grad_scores = (probs * (grad_probs - inner)).astype(LOW)
    grad_q = jnp.einsum("hqk,khd->qhd", grad_scores, keyset, preferred_element_type=jnp.float32)
    grad_k = jnp.einsum("hqk,qhd->khd", grad_scores, queries, preferred_element_type=jnp.float32)
    grad_v = jnp.einsum("hqk,qhd->khd", probs.astype(LOW), grad_out, preferred_element_type=jnp.float32)
    return (grad_q * scale).astype(LOW), (grad_k * scale).astype(LOW), grad_v.astype(LOW)


def gelu(value):
    return jax.nn.gelu(value, approximate=False)


def adamw(weight, mean, square, grad, factor):
    step = grad * factor
    mean_new = beta_first * mean + (1.0 - beta_first) * step
    square_new = beta_second * square + (1.0 - beta_second) * step * step
    mean_hat = mean_new / (1.0 - beta_first**ADAM_STEP)
    square_hat = square_new / (1.0 - beta_second**ADAM_STEP)
    weight_new = weight - learn_rate * (
        mean_hat / (jnp.sqrt(square_hat) + adam_epsilon) + decay_weight * weight
    )
    return (weight_new, mean_new, square_new)


def body(
    token_ids,
    segment_ids,
    completions,
    embedding,
    unembedding,
    query_key_value_weight,
    attention_output_weight,
    up_projection,
    down_projection,
    vectors,
    embedding_mean,
    unembedding_mean,
    input_proj_mean,
    output_proj_mean,
    up_proj_mean,
    down_proj_mean,
    vectors_mean,
    embedding_square,
    unembedding_square,
    input_proj_square,
    output_proj_square,
    up_proj_square,
    down_proj_square,
    vectors_square,
):
    tokens = token_ids.shape[1]
    picks = completions.shape[1]
    seq_index = lax.axis_index("seq")
    fsdp_index = lax.axis_index("fsdp")
    groups = lax.axis_size("seq")
    members = lax.axis_size("fsdp")
    length = groups * tokens
    columns = embedding.shape[1]
    rows = vectors.shape[0]
    heads = HEADS // groups
    width = heads * HEAD_DIM
    hidden = up_projection.shape[2] // groups

    local_ids = token_ids[0]
    chosen_rows = completions[0] - seq_index * tokens
    pick_hot = chosen_rows[:, None] == jnp.arange(tokens)[None, :]
    next_hot = (chosen_rows + 1)[:, None] == jnp.arange(tokens)[None, :]
    local_targets = jnp.sum(jnp.where(next_hot, local_ids[None, :], 0), axis=1)
    small = jnp.concatenate(
        [
            local_ids.astype(jnp.float32),
            segment_ids[0].astype(jnp.float32),
            completions[0].astype(jnp.float32),
            local_targets.astype(jnp.float32),
            lax.reduce_precision(vectors, 8, 7).reshape(-1),
        ]
    )
    extent = small.shape[0]
    padded = -(-extent // 1024) * 1024
    small = jnp.pad(small, (0, padded - extent)).reshape(-1, 128)
    (small_all,) = exchange([small], [True], BOTH, 0, "gather_small")
    small_all = small_all.reshape(groups * members, padded)
    cut = [tokens, 2 * tokens, 2 * tokens + picks, 2 * tokens + 2 * picks]
    all_ids = small_all[:, : cut[0]].astype(jnp.int32).reshape(-1)
    mine = small_all.reshape(groups, members, padded)
    mine = lax.dynamic_index_in_dim(mine, fsdp_index, 1, keepdims=False)
    segments = mine[:, cut[0] : cut[1]].astype(jnp.int32).reshape(-1)
    chosen_places = mine[:, cut[1] : cut[2]].astype(jnp.int32).reshape(-1)
    all_targets = small_all[:, cut[2] : cut[3]].astype(jnp.int32).reshape(-1)
    params = small_all[:, cut[3] : extent].reshape(groups * members, rows, columns)
    params = params.transpose(1, 0, 2).reshape(rows, D)

    local = query_key_value_weight.shape[1]
    wide = query_key_value_weight.astype(LOW).reshape(LAYERS, local, 3, groups, width)
    wide = wide.transpose(3, 0, 1, 2, 4).reshape(groups, LAYERS * local, 3 * width)
    tall = up_projection.astype(LOW).reshape(LAYERS, local, groups, hidden)
    tall = tall.transpose(2, 0, 1, 3).reshape(groups, LAYERS * local, hidden)
    wide, tall = exchange([wide, tall], [False, False], ("seq",), 5, "part_weights")
    wide = wide.reshape(groups, LAYERS, local, 3 * width)
    tall = tall.reshape(groups, LAYERS, local, hidden)
    wide_all = lax.all_gather(wide.reshape(-1, 3 * width), "fsdp", axis=0, tiled=False)
    wide_all = wide_all.reshape(members, groups, LAYERS, local, 3 * width)
    inner = down_projection.shape[1]

    def fetch(depth):
        block = jnp.concatenate(
            [
                tall[:, depth].reshape(groups * local, hidden),
                down_projection[depth].astype(LOW),
                attention_output_weight[depth].astype(LOW),
            ]
        )
        block = lax.all_gather(block, "fsdp", axis=0, tiled=False)
        up = block[:, : groups * local].reshape(members, groups, local, hidden)
        up = up.transpose(1, 0, 2, 3).reshape(D, hidden)
        down = block[:, groups * local : groups * local + inner].reshape(members * inner, D)
        out = block[:, groups * local + inner :].reshape(members * local, D)
        qkv = wide_all[:, :, depth].transpose(1, 0, 2, 3).reshape(D, 3 * width)
        return qkv, out, up, down

    weights = [fetch(depth) for depth in range(LAYERS)]

    def part(vector_rows, size):
        return lax.dynamic_slice_in_dim(vector_rows, seq_index * size, size, axis=-1)

    def biases(depth):
        base = params[13 * depth : 13 * depth + 13]
        qkv_b = part(base[4:7], width).reshape(-1)
        up_b = part(base[8:12].reshape(-1), hidden)
        return qkv_b, up_b

    picked = jnp.take(embedding.astype(LOW), all_ids, axis=0)
    picked = picked.reshape(groups * members, tokens, columns).transpose(0, 2, 1)
    (arrived,) = exchange([picked], [False], BOTH, 1, "send_rows")
    start_own = arrived.reshape(D, tokens).T

    places = jnp.arange(length)
    cosine, sine = angles(places)
    pick_cosine, pick_sine = angles(chosen_places)
    allowed = seen(places, segments, segments)
    pick_segments = jnp.sum(
        jnp.where(chosen_places[:, None] == places[None, :], segments[None, :], 0), axis=1
    )
    pick_allowed = seen(chosen_places, pick_segments, segments)

    start = gather_rows(start_own, "seq").astype(jnp.float32)
    base = params[:13]
    qkv_b, up_b = biases(0)
    qkv_w, out_w, up_w, down_w = weights[0]
    unit0, scale0 = normalized(start)
    first0 = (unit0 * base[0] + base[1]).astype(LOW)
    second0 = (unit0 * base[2] + base[3]).astype(LOW)
    raw = (dot_plain(first0, qkv_w) + qkv_b).reshape(length, 3, heads, HEAD_DIM)
    query0 = rotate(raw[:, 0], cosine, sine).astype(LOW)
    key0 = rotate(raw[:, 1], cosine, sine).astype(LOW)
    value0 = raw[:, 2].astype(LOW)
    mixed0, logsum0 = attend_forward(query0, key0, value0, allowed)
    mixed0 = mixed0.reshape(length, width)
    hidden0 = dot_plain(second0, up_w) + up_b
    active0 = gelu(hidden0).astype(LOW)
    partial = dot_plain(mixed0, out_w) + dot_plain(active0, down_w)
    stream = start_own.astype(jnp.float32) + scatter_sum(partial, "seq") + base[7] + base[12]

    base = params[13:26]
    qkv_b, up_b = biases(1)
    qkv_w, out_w, up_w, down_w = weights[1]
    unit1, scale1 = normalized(stream)
    first_own = (unit1 * base[0] + base[1]).astype(LOW)
    stream_pick = jnp.take(stream, chosen_rows, axis=0)
    unit_pick, scale_pick = normalized(stream_pick)
    first_pick = (unit_pick * base[0] + base[1]).astype(LOW)
    second_pick = (unit_pick * base[2] + base[3]).astype(LOW)
    first1 = gather_rows(first_own, "seq")
    pair = gather_rows(jnp.stack([first_pick, second_pick], axis=1), "seq")
    first1_pick, second1 = pair[:, 0], pair[:, 1]
    raw_q = (dot_plain(first1_pick, qkv_w[:, :width]) + qkv_b[:width]).reshape(-1, heads, HEAD_DIM)
    raw_kv = (dot_plain(first1, qkv_w[:, width:]) + qkv_b[width:]).reshape(length, 2, heads, HEAD_DIM)
    query1 = rotate(raw_q, pick_cosine, pick_sine).astype(LOW)
    key1 = rotate(raw_kv[:, 0], cosine, sine).astype(LOW)
    value1 = raw_kv[:, 1].astype(LOW)
    mixed1, logsum1 = attend_forward(query1, key1, value1, pick_allowed)
    mixed1 = mixed1.reshape(-1, width)
    hidden1 = dot_plain(second1, up_w) + up_b
    active1 = gelu(hidden1).astype(LOW)
    partial = dot_plain(mixed1, out_w) + dot_plain(active1, down_w)
    final_in = stream_pick + scatter_sum(partial, "seq") + base[7] + base[12]

    final_gain, final_shift = params[13 * LAYERS], params[13 * LAYERS + 1]
    unit_f, scale_f = normalized(final_in)
    chosen = (unit_f * final_gain + final_shift).astype(LOW)
    group_rows = gather_rows(chosen, "fsdp")
    all_rows = gather_rows(group_rows, "seq")
    table = unembedding.astype(LOW)
    vocab_rows = table.shape[0]
    row_count = all_rows.shape[0]
    goal = all_targets - fsdp_index * vocab_rows
    vocab_iota = jnp.arange(vocab_rows)
    logits = dot_right(all_rows, table)
    top = jnp.max(logits, axis=-1)
    total = jnp.sum(jnp.exp(logits - top[:, None]), axis=-1)
    hit = jnp.sum(jnp.where(vocab_iota[None, :] == goal[:, None], logits, 0.0), axis=-1)
    stats = jnp.stack([top, total, hit]).reshape(-1, 128)
    (stats,) = exchange([stats], [True], ("fsdp",), 2, "gather_stats")
    stats = stats.reshape(members, 3, row_count)
    best = jnp.max(stats[:, 0], axis=0)
    summed = jnp.sum(stats[:, 1] * jnp.exp(stats[:, 0] - best[None]), axis=0)
    logsumexp = best + jnp.log(summed)
    loss = jnp.sum(logsumexp - jnp.sum(stats[:, 2], axis=0)) / row_count
    onehot = jnp.where(vocab_iota[None, :] == goal[:, None], 1.0, 0.0)
    grad_logits = ((jnp.exp(logits - logsumexp[:, None]) - onehot) / row_count).astype(LOW)
    own_logits = lax.dynamic_slice_in_dim(
        grad_logits, seq_index * group_rows.shape[0], group_rows.shape[0], 0
    )
    grad_chosen = scatter_sum(dot_plain(own_logits, table), "fsdp")
    grad_table = dot_left(grad_logits, all_rows)

    grad_gain = jnp.sum(grad_chosen * unit_f, axis=0)
    grad_shift = jnp.sum(grad_chosen, axis=0)
    grad_final = norm_back(unit_f, scale_f, grad_chosen * final_gain)
    low_own = grad_final.astype(LOW)
    bias1 = jnp.sum(low_own.astype(jnp.float32), axis=0)
    grad_low = gather_rows(low_own, "seq")
    grad_active = dot_right(grad_low, down_w)
    _, pull = jax.vjp(gelu, hidden1)
    grad_hidden = pull(grad_active)[0].astype(LOW)
    grad_mixed = dot_right(grad_low, out_w).astype(LOW).reshape(-1, heads, HEAD_DIM)
    grad_q, grad_k, grad_v = attend_backward(query1, key1, value1, pick_allowed, logsum1, grad_mixed)
    raw_gq = rotate_back(grad_q.astype(jnp.float32), pick_cosine, pick_sine).astype(LOW)
    raw_gk = rotate_back(grad_k.astype(jnp.float32), cosine, sine).astype(LOW)
    raw_gq = raw_gq.reshape(-1, width)
    spread_hot = (places[:, None] == chosen_places[None, :]).astype(LOW)
    full_gq = dot_plain(spread_hot, raw_gq).astype(LOW)
    raw_grad1 = jnp.concatenate(
        [full_gq, raw_gk.reshape(length, width), grad_v.reshape(length, width)], axis=1
    )
    part_qkv1 = dot_left(first1, raw_grad1)
    part_out1 = dot_left(mixed1, grad_low)
    part_up1 = dot_left(second1, grad_hidden)
    part_down1 = dot_left(active1, grad_low)
    qkv_bias1 = jnp.sum(raw_grad1.astype(jnp.float32), axis=0)
    up_bias1 = jnp.sum(grad_hidden.astype(jnp.float32), axis=0)
    grad_second = scatter_sum(dot_right(grad_hidden, up_w), "seq")
    grad_first = scatter_sum(dot_right(raw_grad1, qkv_w), "seq")
    gain_rows1 = [
        jnp.sum(grad_first * unit1, axis=0),
        jnp.sum(grad_first, axis=0),
        jnp.sum(grad_second * unit_pick, axis=0),
        jnp.sum(grad_second, axis=0),
    ]
    back_pick = norm_back(unit_pick, scale_pick, grad_second * base[2]) + grad_final
    grad_stream = norm_back(unit1, scale1, grad_first * base[0])
    grad_stream = grad_stream.at[chosen_rows].add(back_pick)

    base = params[:13]
    qkv_w, out_w, up_w, down_w = weights[0]
    low_own = grad_stream.astype(LOW)
    bias0 = jnp.sum(low_own.astype(jnp.float32), axis=0)
    grad_low = gather_rows(low_own, "seq")
    grad_active = dot_right(grad_low, down_w)
    _, pull = jax.vjp(gelu, hidden0)
    grad_hidden = pull(grad_active)[0].astype(LOW)
    grad_mixed = dot_right(grad_low, out_w).astype(LOW).reshape(length, heads, HEAD_DIM)
    grad_q, grad_k, grad_v = attend_backward(query0, key0, value0, allowed, logsum0, grad_mixed)
    raw_gq = rotate_back(grad_q.astype(jnp.float32), cosine, sine).astype(LOW)
    raw_gk = rotate_back(grad_k.astype(jnp.float32), cosine, sine).astype(LOW)
    raw_grad0 = jnp.stack([raw_gq, raw_gk, grad_v], axis=1).reshape(length, 3 * width)
    part_qkv0 = dot_left(first0, raw_grad0)
    part_out0 = dot_left(mixed0, grad_low)
    part_up0 = dot_left(second0, grad_hidden)
    part_down0 = dot_left(active0, grad_low)
    qkv_bias0 = jnp.sum(raw_grad0.astype(jnp.float32), axis=0)
    up_bias0 = jnp.sum(grad_hidden.astype(jnp.float32), axis=0)
    grad_first = dot_right(raw_grad0, qkv_w)
    grad_second = dot_right(grad_hidden, up_w)
    gain_rows0 = [
        jnp.sum(grad_first * unit0, axis=0),
        jnp.sum(grad_first, axis=0),
        jnp.sum(grad_second * unit0, axis=0),
        jnp.sum(grad_second, axis=0),
    ]
    own = seq_index * tokens
    grad_unit = scatter_sum(grad_first * base[0] + grad_second * base[2], "seq")
    grad_stream = grad_stream + norm_back(
        lax.dynamic_slice_in_dim(unit0, own, tokens, 0),
        lax.dynamic_slice_in_dim(scale0, own, tokens, 0),
        grad_unit,
    )

    def to_owner(part_qkv, part_out, part_up, part_down):
        def by_owner(value):
            value = value.reshape(groups, members, local, value.shape[1])
            return value.transpose(1, 0, 2, 3).reshape(members, groups * local, value.shape[3])

        block = jnp.concatenate(
            [
                by_owner(part_up),
                part_down.reshape(members, inner, D),
                part_out.reshape(members, local, D),
            ],
            axis=1,
        )
        block = lax.psum_scatter(block.reshape(-1, D), "fsdp", scatter_dimension=0, tiled=True)
        qkv = lax.psum_scatter(
            by_owner(part_qkv).reshape(-1, 3 * width), "fsdp", scatter_dimension=0, tiled=True
        )
        up = block[: groups * local].reshape(groups, local, hidden)
        down = block[groups * local : groups * local + inner]
        out = block[groups * local + inner :]
        return qkv.reshape(groups, local, 3 * width), out, up, down

    parts1 = to_owner(part_qkv1, part_out1, part_up1, part_down1)
    parts0 = to_owner(part_qkv0, part_out0, part_up0, part_down0)
    moved = exchange(
        [parts0[0], parts1[0], parts0[2], parts1[2]], [False] * 4, ("seq",), 6, "part_grads"
    )

    def owned(depth):
        qkv = moved[depth].reshape(groups, local, 3, width)
        qkv = qkv.transpose(1, 2, 0, 3).reshape(local, 3 * D)
        up = moved[LAYERS + depth].transpose(1, 0, 2).reshape(local, groups * hidden)
        other = (parts0, parts1)[depth]
        return qkv, other[1], up, other[3]

    layer_grads = [owned(depth) for depth in range(LAYERS)]

    def whole(vector, size, count):
        spot = jnp.zeros((count, groups, size), jnp.float32)
        spot = lax.dynamic_update_slice(spot, vector.reshape(count, 1, size), (0, seq_index, 0))
        return spot.reshape(count, groups * size)

    def vector_rows(gain_rows, qkv_bias, up_bias, bias):
        return jnp.concatenate(
            [
                jnp.stack(gain_rows),
                whole(qkv_bias, width, 3),
                bias[None],
                whole(up_bias, hidden, 1).reshape(-1, D),
                bias[None],
            ]
        )

    vector_grad = jnp.concatenate(
        [
            vector_rows(gain_rows0, qkv_bias0, up_bias0, bias0),
            vector_rows(gain_rows1, qkv_bias1, up_bias1, bias1),
            jnp.stack([grad_gain, grad_shift]),
        ]
    )
    vector_send = vector_grad.reshape(rows, groups * members, columns).transpose(1, 0, 2)
    vector_send = vector_send.reshape(groups * members, rows * columns)
    spare = -(rows * columns) % 1024
    vector_send = jnp.pad(vector_send, ((0, 0), (0, spare))).reshape(groups * members, -1, 128)
    row_send = grad_stream.astype(LOW).T.reshape(groups * members, columns, tokens)
    row_back, vector_back = exchange(
        [row_send, vector_send], [False, False], BOTH, 3, "return_rows"
    )
    grad_vectors = jnp.sum(vector_back, axis=0).reshape(-1)[: rows * columns].reshape(rows, columns)
    row_back = row_back.transpose(0, 2, 1)
    grad_embedding = jax.ops.segment_sum(
        row_back.reshape(-1, columns).astype(jnp.float32), all_ids, num_segments=embedding.shape[0]
    )

    grads = (
        grad_embedding,
        grad_table,
        jnp.stack([layer_grads[depth][0] for depth in range(LAYERS)]),
        jnp.stack([layer_grads[depth][1] for depth in range(LAYERS)]),
        jnp.stack([layer_grads[depth][2] for depth in range(LAYERS)]),
        jnp.stack([layer_grads[depth][3] for depth in range(LAYERS)]),
        grad_vectors,
    )
    squares = jnp.zeros((), jnp.float32)
    for index in range(7):
        term = jnp.sum(grads[index] * grads[index])
        if index == 1:
            term = jnp.where(seq_index == 0, term, 0.0)
        squares = squares + term
    (norm_parts,) = exchange(
        [jnp.broadcast_to(squares, (8, 128))], [True], BOTH, 4, "gather_norm"
    )
    grad_norm = jnp.sqrt(jnp.sum(norm_parts[:, 0, 0]))
    factor = jnp.minimum(1.0, clip_limit / grad_norm)
    weights_all = (
        embedding,
        unembedding,
        query_key_value_weight,
        attention_output_weight,
        up_projection,
        down_projection,
        vectors,
    )
    means = (
        embedding_mean,
        unembedding_mean,
        input_proj_mean,
        output_proj_mean,
        up_proj_mean,
        down_proj_mean,
        vectors_mean,
    )
    seconds = (
        embedding_square,
        unembedding_square,
        input_proj_square,
        output_proj_square,
        up_proj_square,
        down_proj_square,
        vectors_square,
    )
    result = [
        adamw(weights_all[index], means[index], seconds[index], grads[index], factor)
        for index in range(7)
    ]
    return (loss, grad_norm) + tuple(result[index][kind] for kind in range(3) for index in range(7))


def solution(mesh):
    state = (
        P(None, BOTH),
        P("fsdp", None),
        P(None, BOTH, None),
        P(None, BOTH, None),
        P(None, BOTH, None),
        P(None, BOTH, None),
        P(None, BOTH),
    )
    in_specs = (P("fsdp", "seq"),) * 3 + state * 3
    out_specs = (P(), P()) + state * 3
    return jax.shard_map(body, mesh=mesh, in_specs=in_specs, out_specs=out_specs, check_vma=False)
```

```python
import functools

import jax
import jax.numpy as jnp
from jax import lax
from jax.experimental import pallas as pl
from jax.experimental.pallas import tpu as pltpu
from jax.sharding import PartitionSpec as P

HEADS = 12
HEAD_DIM = 64
D = 768
ROT = 16
LAYERS = 2
ADAM_STEP = 3

norm_epsilon = 1e-05
clip_limit = 0.25
learn_rate = 0.03
beta_first = 0.9
beta_second = 0.95
adam_epsilon = 1e-08
decay_weight = 0.1
masked_score = -1000000000.0

MESH = pl.DeviceIdType.MESH
BOTH = ("seq", "fsdp")
LANES = 128
PACK = 4
LOW = jnp.bfloat16


def peer_of(step, axes, sizes):
    here = 0
    count = 1
    for axis, size in zip(axes, sizes):
        here = here * size + lax.axis_index(axis)
        count = count * size
    there = lax.rem(here + step, count)
    coords = {}
    rest = there
    for axis, size in reversed(list(zip(axes, sizes))):
        coords[axis] = lax.rem(rest, size)
        rest = lax.div(rest, size)
    return here, there, coords


def exchange_kernel(axes, sizes, gather, count, *refs):
    arrays = len(gather)
    ins, outs = refs[:arrays], refs[arrays : 2 * arrays]
    send, recv, own = refs[2 * arrays :]
    barrier = pltpu.get_barrier_semaphore()

    def greet(step, carry):
        _, _, coords = peer_of(step, axes, sizes)
        pl.semaphore_signal(barrier, inc=1, device_id=coords, device_id_type=MESH)
        return carry

    lax.fori_loop(1, count, greet, 0)
    pl.semaphore_wait(barrier, count - 1)
    here, _, _ = peer_of(0, axes, sizes)

    def copy(which, step):
        _, there, coords = peer_of(step, axes, sizes)
        source = ins[which] if gather[which] else ins[which].at[there]
        return pltpu.make_async_remote_copy(
            source,
            outs[which].at[here],
            send.at[which, step],
            recv.at[which, step],
            device_id=coords,
            device_id_type=MESH,
        )

    def begin(step, carry):
        for which in range(arrays):
            copy(which, step).start()
        return carry

    def finish(step, carry):
        for which in range(arrays):
            copy(which, step).wait()
        return carry

    lax.fori_loop(1, count, begin, 0)
    locals_ = [
        pltpu.make_async_copy(
            ins[which] if gather[which] else ins[which].at[here],
            outs[which].at[here],
            own.at[which],
        )
        for which in range(arrays)
    ]
    for item in locals_:
        item.start()
    for item in locals_:
        item.wait()
    lax.fori_loop(1, count, finish, 0)


def exchange(values, gather, axes, ident, name):
    sizes = tuple(lax.axis_size(axis) for axis in axes)
    count = 1
    for size in sizes:
        count = count * size
    shapes = [
        jax.ShapeDtypeStruct(((count,) + value.shape) if every else value.shape, value.dtype)
        for value, every in zip(values, gather)
    ]
    arrays = len(values)
    space = pl.BlockSpec(memory_space=pltpu.VMEM)
    return pl.pallas_call(
        functools.partial(exchange_kernel, axes, sizes, tuple(gather), count),
        out_shape=shapes,
        in_specs=[space] * arrays,
        out_specs=[space] * arrays,
        scratch_shapes=[
            pltpu.SemaphoreType.DMA((arrays, count)),
            pltpu.SemaphoreType.DMA((arrays, count)),
            pltpu.SemaphoreType.DMA((arrays,)),
        ],
        compiler_params=pltpu.CompilerParams(collective_id=ident, has_side_effects=True),
        name=name,
    )(*values)


def ring_pairs(size, step):
    return [(place, (place + step) % size) for place in range(size)]


def gather_rows(block, axis):
    size = lax.axis_size(axis)
    here = lax.axis_index(axis)
    out = jnp.zeros((size,) + block.shape, block.dtype)
    out = lax.dynamic_update_index_in_dim(out, block, here, 0)
    for step in range(1, size):
        piece = lax.ppermute(block, axis, ring_pairs(size, step))
        out = lax.dynamic_update_index_in_dim(out, piece, lax.rem(here - step + size, size), 0)
    return out.reshape((size * block.shape[0],) + block.shape[1:])


def gather_chosen_kernel(groups, chips, x_ref, out_ref, send, recv, own):
    seq = lax.axis_index("seq")
    fsdp = lax.axis_index("fsdp")
    chip, core = lax.div(fsdp, 2), lax.rem(fsdp, 2)

    def along(step):
        return {"seq": seq, "fsdp": lax.rem(chip + step, chips) * 2 + core}

    def across(step):
        return {"seq": lax.rem(seq + step, groups), "fsdp": fsdp}

    other = {"seq": seq, "fsdp": chip * 2 + 1 - core}
    barrier = pltpu.get_barrier_semaphore()
    peers = [along(step) for step in range(1, chips)] + [across(step) for step in range(1, groups)]
    peers.append(other)
    for peer in peers:
        pl.semaphore_signal(barrier, inc=1, device_id=peer, device_id_type=MESH)
    pl.semaphore_wait(barrier, len(peers))
    mine = out_ref.at[core, seq, chip]
    local = pltpu.make_async_copy(x_ref, mine, own)
    local.start()
    first = [
        pltpu.make_async_remote_copy(
            x_ref, mine, send.at[step], recv.at[step], device_id=along(step), device_id_type=MESH
        )
        for step in range(1, chips)
    ]
    for item in first:
        item.start()
    local.wait()
    for item in first:
        item.wait()
    line = out_ref.at[core, seq]
    second = [
        pltpu.make_async_remote_copy(
            line,
            line,
            send.at[chips + step],
            recv.at[chips + step],
            device_id=across(step),
            device_id_type=MESH,
        )
        for step in range(1, groups)
    ]
    for item in second:
        item.start()
    for item in second:
        item.wait()
    half = out_ref.at[core]
    third = pltpu.make_async_remote_copy(
        half, half, send.at[0], recv.at[0], device_id=other, device_id_type=MESH
    )
    third.start()
    third.wait()


def gather_chosen(rows):
    groups, members = lax.axis_size("seq"), lax.axis_size("fsdp")
    chips = members // 2
    space = pl.BlockSpec(memory_space=pltpu.VMEM)
    return pl.pallas_call(
        functools.partial(gather_chosen_kernel, groups, chips),
        out_shape=jax.ShapeDtypeStruct((2, groups, chips) + rows.shape, rows.dtype),
        in_specs=[space],
        out_specs=space,
        scratch_shapes=[
            pltpu.SemaphoreType.DMA((chips + groups,)),
            pltpu.SemaphoreType.DMA((chips + groups,)),
            pltpu.SemaphoreType.DMA,
        ],
        compiler_params=pltpu.CompilerParams(collective_id=7, has_side_effects=True),
        name="gather_chosen",
    )(rows)


def return_chosen(partial):
    members = lax.axis_size("fsdp")
    chips = members // 2
    fsdp = lax.axis_index("fsdp")
    chip, core = lax.div(fsdp, 2), lax.rem(fsdp, 2)
    away = lax.dynamic_index_in_dim(partial, 1 - core, 0, keepdims=False)
    away = lax.ppermute(away, "fsdp", [(place, place ^ 1) for place in range(members)])
    pair = lax.dynamic_index_in_dim(partial, core, 0, keepdims=False) + away
    total = lax.dynamic_index_in_dim(pair, chip, 0, keepdims=False)
    for step in range(1, chips):
        piece = lax.dynamic_index_in_dim(pair, lax.rem(chip + step, chips), 0, keepdims=False)
        pairs = [(place, (place // 2 + step) % chips * 2 + place % 2) for place in range(members)]
        total = total + lax.ppermute(piece, "fsdp", pairs)
    return total


def scatter_sum(partial, axis):
    size = lax.axis_size(axis)
    here = lax.axis_index(axis)
    blocks = partial.reshape((size, partial.shape[0] // size) + partial.shape[1:])
    pieces = []
    for step in range(1, size):
        piece = lax.dynamic_index_in_dim(blocks, lax.rem(here + step, size), 0, keepdims=False)
        pieces.append(lax.ppermute(piece, axis, ring_pairs(size, step)))
    total = lax.dynamic_index_in_dim(blocks, here, 0, keepdims=False)
    for piece in pieces:
        total = total + piece
    return total


def packed_rows(vocab):
    return -(-vocab // (PACK * LANES)) * LANES

def add_rows_kernel(vocab, columns, copies, at_ref, which_ref, rows_ref, out_ref, square_ref, placed, *totals):
    slot = LANES // PACK
    deep = packed_rows(vocab)
    tiles = deep // LANES
    last = -(-vocab // LANES)

    def clear(step, carry):
        for total in totals:
            total[pl.ds(pl.multiple_of(step * LANES, LANES), LANES), :] = jnp.zeros((LANES, LANES), jnp.float32)
        return carry

    lax.fori_loop(0, tiles, clear, 0)
    chunks = rows_ref.shape[0]

    def chunk(step, carry):
        block = rows_ref[step].astype(jnp.float32)
        which = which_ref[pl.ds(step, 1), :]
        blank = jnp.zeros((slot - columns, LANES), jnp.float32)
        pieces = []
        for place in range(PACK):
            pieces += [jnp.where(which == place, block, 0.0), blank]
        placed[...] = jnp.concatenate(pieces, axis=0).T
        base = step * LANES

        def add(item, inner):
            first = item * 8
            for k in range(8):
                token = first + k
                total = totals[k % copies]
                at = at_ref[base + token]
                total[pl.ds(at, 1), :] = total[pl.ds(at, 1), :] + placed[pl.ds(token, 1), :]
            return inner

        lax.fori_loop(0, LANES // 8, add, 0)
        return carry

    lax.fori_loop(0, chunks, chunk, 0)

    def tile(step, square):
        spot = pl.ds(pl.multiple_of(step * LANES, LANES), LANES)
        value = totals[0][spot, :]
        for total in totals[1:]:
            value = value + total[spot, :]
        square = square + jnp.sum((value * value).reshape(LANES // 8, 8, LANES), axis=0)
        value = value.T
        for place in range(PACK):
            where = place * tiles + step

            @pl.when(where < last)
            def _():
                out_ref[:, pl.ds(pl.multiple_of(where * LANES, LANES), LANES)] = value[
                    place * slot : place * slot + columns
                ]

        return square

    square_ref[...] = lax.fori_loop(0, tiles, tile, jnp.zeros((8, LANES), jnp.float32))


def add_rows(ids, rows, vocab):
    chunks, columns, _ = rows.shape
    deep = packed_rows(vocab)
    which = ids // deep
    at = ids - which * deep
    copies = 4
    wide = -(-vocab // LANES) * LANES
    vm = pl.BlockSpec(memory_space=pltpu.VMEM)
    return pl.pallas_call(
        functools.partial(add_rows_kernel, vocab, columns, copies),
        out_shape=[
            jax.ShapeDtypeStruct((columns, wide), jnp.float32),
            jax.ShapeDtypeStruct((8, LANES), jnp.float32),
        ],
        in_specs=[pl.BlockSpec(memory_space=pltpu.SMEM), vm, vm],
        out_specs=[vm, vm],
        scratch_shapes=[pltpu.VMEM((LANES, LANES), jnp.float32)]
        + [pltpu.VMEM((deep, LANES), jnp.float32)] * copies,
        compiler_params=pltpu.CompilerParams(vmem_limit_bytes=60 * 1024 * 1024),
        name="add_rows",
    )(at, which.reshape(chunks, LANES), rows)


def take_rows_kernel(vocab, columns, at_ref, which_ref, table_ref, out_ref, packed, taken):
    slot = LANES // PACK
    deep = packed_rows(vocab)
    tiles = deep // LANES
    last = -(-vocab // LANES)

    def fill(step, carry):
        blank = jnp.zeros((slot - columns, LANES), jnp.float32)
        pieces = []
        for place in range(PACK):
            where = jnp.minimum(place * tiles + step, last - 1)
            block = table_ref[:, pl.ds(pl.multiple_of(where * LANES, LANES), LANES)]
            pieces += [block, blank]
        packed[pl.ds(pl.multiple_of(step * LANES, LANES), LANES), :] = jnp.concatenate(pieces, axis=0).T
        return carry

    lax.fori_loop(0, tiles, fill, 0)
    chunks = out_ref.shape[0]

    def chunk(step, carry):
        base = step * LANES

        def copy(item, inner):
            first = pl.multiple_of(item * 8, 8)
            got = [packed[pl.ds(at_ref[base + first + k], 1), :] for k in range(8)]
            taken[pl.ds(first, 8), :] = jnp.concatenate(got, axis=0)
            return inner

        lax.fori_loop(0, LANES // 8, copy, 0)
        which = which_ref[pl.ds(step, 1), :]
        value = taken[...].T
        result = jnp.zeros((columns, LANES), jnp.float32)
        for place in range(PACK):
            result = jnp.where(which == place, value[place * slot : place * slot + columns], result)
        out_ref[step] = result.astype(out_ref.dtype)
        return carry

    lax.fori_loop(0, chunks, chunk, 0)


def take_rows(ids, table):
    columns, vocab = table.shape
    wide = -(-vocab // LANES) * LANES
    if wide != vocab:
        table = jnp.pad(table, ((0, 0), (0, wide - vocab)))
    deep = packed_rows(vocab)
    which = ids // deep
    at = ids - which * deep
    chunks = ids.shape[0] // LANES
    vm = pl.BlockSpec(memory_space=pltpu.VMEM)
    return pl.pallas_call(
        functools.partial(take_rows_kernel, vocab, columns),
        out_shape=jax.ShapeDtypeStruct((chunks, columns, LANES), LOW),
        in_specs=[pl.BlockSpec(memory_space=pltpu.SMEM), vm, vm],
        out_specs=vm,
        scratch_shapes=[
            pltpu.VMEM((deep, LANES), jnp.float32),
            pltpu.VMEM((LANES, LANES), jnp.float32),
        ],
        compiler_params=pltpu.CompilerParams(vmem_limit_bytes=40 * 1024 * 1024),
        name="take_rows",
    )(at, which.reshape(chunks, LANES), table)


def vocab_block(rows, limit):
    best = rows
    for size in range(8, min(rows, limit) + 1, 8):
        if rows % size == 0:
            best = size
    return best

def row_tile(size, count):
    tile = count
    while size * tile * 4 > 10 * 1024 * 1024:
        tile = tile // 2
    return tile


def score_kernel(span, rows_ref, table_ref, logits_ref, top_ref, total_ref):
    table = table_ref[...].astype(LOW)

    @pl.when(pl.program_id(1) == 0)
    def _():
        top_ref[...] = jnp.full(top_ref.shape, -jnp.inf, jnp.float32)
        total_ref[...] = jnp.zeros(total_ref.shape, jnp.float32)

    def part(item, carry):
        spot = pl.ds(pl.multiple_of(item * span, span), span)
        value = lax.dot_general(
            table, rows_ref[spot, :], (((1,), (1,)), ((), ())), preferred_element_type=jnp.float32
        )
        logits_ref[:, spot] = value
        old = top_ref[:, spot]
        new = jnp.maximum(old, jnp.max(value, axis=0, keepdims=True))
        total_ref[:, spot] = total_ref[:, spot] * jnp.exp(old - new) + jnp.sum(
            jnp.exp(value - new), axis=0, keepdims=True
        )
        top_ref[:, spot] = new
        return carry

    lax.fori_loop(0, rows_ref.shape[0] // span, part, 0, unroll=True)


def score(all_rows, table):
    count, depth = all_rows.shape
    vocab = table.shape[0]
    size = vocab_block(vocab, 1100)
    tile = row_tile(size, count)
    span = min(512, tile)
    row = jax.ShapeDtypeStruct((1, count), jnp.float32)
    return pl.pallas_call(
        functools.partial(score_kernel, span),
        grid=(count // tile, vocab // size),
        out_shape=[jax.ShapeDtypeStruct((vocab, count), jnp.float32), row, row],
        in_specs=[
            pl.BlockSpec((tile, depth), lambda j, i: (j, 0)),
            pl.BlockSpec((size, depth), lambda j, i: (i, 0)),
        ],
        out_specs=[
            pl.BlockSpec((size, tile), lambda j, i: (i, j)),
            pl.BlockSpec((1, tile), lambda j, i: (0, j)),
            pl.BlockSpec((1, tile), lambda j, i: (0, j)),
        ],
        compiler_params=pltpu.CompilerParams(vmem_limit_bytes=60 * 1024 * 1024),
        name="score",
    )(all_rows, table)


def table_grad_kernel(
    span,
    group,
    count,
    rows_ref,
    table_ref,
    logits_ref,
    goal_ref,
    lse_ref,
    start_ref,
    which_ref,
    grad_ref,
    chosen_ref,
    square_ref,
    hit_ref,
    low,
):
    step, turn = pl.program_id(0), pl.program_id(1)
    size = table_ref.shape[0]
    tile = rows_ref.shape[0]

    @pl.when((step == 0) & (turn == 0))
    def _():
        chosen_ref[...] = jnp.zeros(chosen_ref.shape, jnp.float32)
        square_ref[...] = jnp.zeros(square_ref.shape, jnp.float32)
        hit_ref[...] = jnp.zeros(hit_ref.shape, jnp.float32)

    place = lax.broadcasted_iota(jnp.int32, (size, span), 0) + (start_ref[0] + step * size)

    def part(item, carry):
        spot = pl.ds(pl.multiple_of(item * span, span), span)
        value = logits_ref[:, spot]
        prob = jnp.exp(value - lse_ref[:, spot])
        match = place == goal_ref[:, spot]
        hit_ref[:, spot] += jnp.sum(jnp.where(match, value, 0.0), axis=0, keepdims=True)
        prob = jnp.where(match, prob - 1.0, prob)
        low[:, spot] = (prob / count).astype(LOW)
        return carry

    lax.fori_loop(0, tile // span, part, 0, unroll=True)
    value = jnp.dot(low[...], rows_ref[...], preferred_element_type=jnp.float32)
    if tile == count:
        grad_ref[...] = value
        square_ref[...] += jnp.sum(value * value, axis=0, keepdims=True)
    else:

        @pl.when(turn == 0)
        def _():
            grad_ref[...] = value

        @pl.when(turn > 0)
        def _():
            grad_ref[...] += value

        @pl.when(turn == count // tile - 1)
        def _():
            square_ref[...] += jnp.sum(grad_ref[...] * grad_ref[...], axis=0, keepdims=True)

    table = table_ref[...].astype(LOW)
    for core in range(2):
        start = which_ref[0] * group + core * (count // 2)

        @pl.when(lax.div(start, tile) == turn)
        def _():
            spot = pl.ds(pl.multiple_of(lax.rem(start, tile), group), group)
            chosen_ref[core * group : (core + 1) * group] += lax.dot_general(
                low[:, spot], table, (((0,), (0,)), ((), ())), preferred_element_type=jnp.float32
            )


def table_grad(all_rows, table, logits, goal, lse, start, which, group):
    count, depth = all_rows.shape
    vocab = table.shape[0]
    size = vocab_block(vocab, 1100)
    tile = row_tile(size, count)
    span = min(512, tile)
    whole = lambda i, j: (0, 0)
    line = pl.BlockSpec((1, tile), lambda i, j: (0, j))
    smem = pl.BlockSpec(memory_space=pltpu.SMEM)
    return pl.pallas_call(
        functools.partial(table_grad_kernel, span, group, count),
        grid=(vocab // size, count // tile),
        out_shape=[
            jax.ShapeDtypeStruct((vocab, depth), jnp.float32),
            jax.ShapeDtypeStruct((2 * group, depth), jnp.float32),
            jax.ShapeDtypeStruct((1, depth), jnp.float32),
            jax.ShapeDtypeStruct((1, tile), jnp.float32),
        ],
        in_specs=[
            pl.BlockSpec((tile, depth), lambda i, j: (j, 0)),
            pl.BlockSpec((size, depth), lambda i, j: (i, 0)),
            pl.BlockSpec((size, tile), lambda i, j: (i, j)),
            line,
            line,
            smem,
            smem,
        ],
        out_specs=[
            pl.BlockSpec((size, depth), lambda i, j: (i, 0)),
            pl.BlockSpec((2 * group, depth), whole),
            pl.BlockSpec((1, depth), whole),
            pl.BlockSpec((1, tile), whole),
        ],
        scratch_shapes=[pltpu.VMEM((size, tile), LOW)],
        compiler_params=pltpu.CompilerParams(vmem_limit_bytes=62 * 1024 * 1024),
        name="table_grad",
    )(
        all_rows,
        table,
        logits,
        goal.reshape(1, count),
        lse.reshape(1, count),
        start.reshape(1),
        which.reshape(1),
    )


def layer_norm(inputs, gain, shift):
    center = inputs - jnp.mean(inputs, axis=-1, keepdims=True)
    spread = jnp.mean(center * center, axis=-1, keepdims=True)
    return center * lax.rsqrt(spread + norm_epsilon) * gain + shift


def normalized(inputs):
    center = inputs - jnp.mean(inputs, axis=-1, keepdims=True)
    spread = jnp.mean(center * center, axis=-1, keepdims=True)
    scale = lax.rsqrt(spread + norm_epsilon)
    return center * scale, scale


def norm_back(unit, scale, grad_unit):
    first = jnp.mean(grad_unit, axis=-1, keepdims=True)
    second = jnp.mean(grad_unit * unit, axis=-1, keepdims=True)
    return scale * (grad_unit - first - unit * second)


def angles(places):
    half = ROT // 2
    freq = 1.0 / 10000.0 ** (jnp.arange(half).astype(jnp.float32) * 2.0 / ROT)
    angle = places.astype(jnp.float32)[:, None] * freq[None, :]
    return jnp.cos(angle)[:, None, :], jnp.sin(angle)[:, None, :]


def rotate(inputs, cosine, sine):
    half = ROT // 2
    first = inputs[..., :half]
    second = inputs[..., half:ROT]
    return jnp.concatenate(
        [first * cosine - second * sine, second * cosine + first * sine, inputs[..., ROT:]], axis=-1
    )


def rotate_back(inputs, cosine, sine):
    return rotate(inputs, cosine, -sine)


def dot_plain(left, right):
    return jnp.dot(left, right, preferred_element_type=jnp.float32)


def dot_left(left, right):
    return lax.dot_general(
        left, right, (((0,), (0,)), ((), ())), preferred_element_type=jnp.float32
    )


def dot_right(left, right):
    return lax.dot_general(
        left, right, (((1,), (1,)), ((), ())), preferred_element_type=jnp.float32
    )


def seen(rowpos, rowseg, segments):
    cols = jnp.arange(segments.shape[0])
    return (cols[None, :] <= rowpos[:, None]) & (segments[None, :] == rowseg[:, None])


def attend_forward(queries, keyset, valueset, allowed):
    scale = queries.shape[-1] ** (-0.5)
    scores = jnp.einsum("qhd,khd->hqk", queries, keyset, preferred_element_type=jnp.float32) * scale
    scores = jnp.where(allowed[None], scores, masked_score)
    top = jnp.max(scores, axis=-1, keepdims=True)
    expo = jnp.exp(scores - top)
    total = jnp.sum(expo, axis=-1, keepdims=True)
    probs = (expo / total).astype(LOW)
    result = jnp.einsum("hqk,khd->qhd", probs, valueset, preferred_element_type=jnp.float32)
    return result.astype(LOW), (top + jnp.log(total))[..., 0]


def attend_backward(queries, keyset, valueset, allowed, logsum, grad_out):
    scale = queries.shape[-1] ** (-0.5)
    scores = jnp.einsum("qhd,khd->hqk", queries, keyset, preferred_element_type=jnp.float32) * scale
    scores = jnp.where(allowed[None], scores, masked_score)
    probs = jnp.exp(scores - logsum[..., None])
    grad_probs = jnp.einsum("qhd,khd->hqk", grad_out, valueset, preferred_element_type=jnp.float32)
    inner = jnp.sum(probs * grad_probs, axis=-1, keepdims=True)
    grad_scores = (probs * (grad_probs - inner)).astype(LOW)
    grad_q = jnp.einsum("hqk,khd->qhd", grad_scores, keyset, preferred_element_type=jnp.float32)
    grad_k = jnp.einsum("hqk,qhd->khd", grad_scores, queries, preferred_element_type=jnp.float32)
    grad_v = jnp.einsum("hqk,qhd->khd", probs.astype(LOW), grad_out, preferred_element_type=jnp.float32)
    return (grad_q * scale).astype(LOW), (grad_k * scale).astype(LOW), grad_v.astype(LOW)


def gelu(value):
    return jax.nn.gelu(value, approximate=False)


def adamw(weight, mean, square, grad, factor):
    step = grad * factor
    mean_new = beta_first * mean + (1.0 - beta_first) * step
    square_new = beta_second * square + (1.0 - beta_second) * step * step
    mean_hat = mean_new / (1.0 - beta_first**ADAM_STEP)
    square_hat = square_new / (1.0 - beta_second**ADAM_STEP)
    weight_new = weight - learn_rate * (
        mean_hat / (jnp.sqrt(square_hat) + adam_epsilon) + decay_weight * weight
    )
    return (weight_new, mean_new, square_new)


def body(
    token_ids,
    segment_ids,
    completions,
    embedding,
    unembedding,
    query_key_value_weight,
    attention_output_weight,
    up_projection,
    down_projection,
    vectors,
    embedding_mean,
    unembedding_mean,
    input_proj_mean,
    output_proj_mean,
    up_proj_mean,
    down_proj_mean,
    vectors_mean,
    embedding_square,
    unembedding_square,
    input_proj_square,
    output_proj_square,
    up_proj_square,
    down_proj_square,
    vectors_square,
):
    tokens = token_ids.shape[1]
    picks = completions.shape[1]
    seq_index = lax.axis_index("seq")
    fsdp_index = lax.axis_index("fsdp")
    groups = lax.axis_size("seq")
    members = lax.axis_size("fsdp")
    length = groups * tokens
    columns = embedding.shape[1]
    rows = vectors.shape[0]
    heads = HEADS // groups
    width = heads * HEAD_DIM
    hidden = up_projection.shape[2] // groups

    local_ids = token_ids[0]
    chosen_rows = completions[0] - seq_index * tokens
    pick_hot = chosen_rows[:, None] == jnp.arange(tokens)[None, :]
    next_hot = (chosen_rows + 1)[:, None] == jnp.arange(tokens)[None, :]
    local_targets = jnp.sum(jnp.where(next_hot, local_ids[None, :], 0), axis=1)
    small = jnp.concatenate(
        [
            local_ids.astype(jnp.float32),
            segment_ids[0].astype(jnp.float32),
            completions[0].astype(jnp.float32),
            local_targets.astype(jnp.float32),
            lax.reduce_precision(vectors, 8, 7).reshape(-1),
        ]
    )
    extent = small.shape[0]
    padded = -(-extent // 1024) * 1024
    small = jnp.pad(small, (0, padded - extent)).reshape(-1, 128)
    (small_all,) = exchange([small], [True], BOTH, 0, "gather_small")
    small_all = small_all.reshape(groups * members, padded)
    cut = [tokens, 2 * tokens, 2 * tokens + picks, 2 * tokens + 2 * picks]
    all_ids = small_all[:, : cut[0]].astype(jnp.int32).reshape(-1)
    mine = small_all.reshape(groups, members, padded)
    mine = lax.dynamic_index_in_dim(mine, fsdp_index, 1, keepdims=False)
    segments = mine[:, cut[0] : cut[1]].astype(jnp.int32).reshape(-1)
    chosen_places = mine[:, cut[1] : cut[2]].astype(jnp.int32).reshape(-1)
    all_targets = small_all[:, cut[2] : cut[3]].astype(jnp.int32).reshape(-1)
    params = small_all[:, cut[3] : extent].reshape(groups * members, rows, columns)
    params = params.transpose(1, 0, 2).reshape(rows, D)

    local = query_key_value_weight.shape[1]
    wide = query_key_value_weight.astype(LOW).reshape(LAYERS, local, 3, groups, width)
    wide = wide.transpose(3, 0, 1, 2, 4).reshape(groups, LAYERS * local, 3 * width)
    tall = up_projection.astype(LOW).reshape(LAYERS, local, groups, hidden)
    tall = tall.transpose(2, 0, 1, 3).reshape(groups, LAYERS * local, hidden)
    wide, tall = exchange([wide, tall], [False, False], ("seq",), 5, "part_weights")
    wide = wide.reshape(groups, LAYERS, local, 3 * width)
    tall = tall.reshape(groups, LAYERS, local, hidden)
    wide_all = lax.all_gather(wide.reshape(-1, 3 * width), "fsdp", axis=0, tiled=False)
    wide_all = wide_all.reshape(members, groups, LAYERS, local, 3 * width)
    inner = down_projection.shape[1]

    def fetch(depth):
        block = jnp.concatenate(
            [
                tall[:, depth].reshape(groups * local, hidden),
                down_projection[depth].astype(LOW),
                attention_output_weight[depth].astype(LOW),
            ]
        )
        block = lax.all_gather(block, "fsdp", axis=0, tiled=False)
        up = block[:, : groups * local].reshape(members, groups, local, hidden)
        up = up.transpose(1, 0, 2, 3).reshape(D, hidden)
        down = block[:, groups * local : groups * local + inner].reshape(members * inner, D)
        out = block[:, groups * local + inner :].reshape(members * local, D)
        qkv = wide_all[:, :, depth].transpose(1, 0, 2, 3).reshape(D, 3 * width)
        return qkv, out, up, down

    weights = [fetch(depth) for depth in range(LAYERS)]

    def part(vector_rows, size):
        return lax.dynamic_slice_in_dim(vector_rows, seq_index * size, size, axis=-1)

    def biases(depth):
        base = params[13 * depth : 13 * depth + 13]
        qkv_b = part(base[4:7], width).reshape(-1)
        up_b = part(base[8:12].reshape(-1), hidden)
        return qkv_b, up_b

    chunks = tokens // LANES
    picked = take_rows(all_ids, lax.reduce_precision(embedding, 8, 7).T)
    picked = picked.reshape(groups * members, chunks, columns, LANES)
    (arrived,) = exchange([picked], [False], BOTH, 1, "send_rows")
    start_own = arrived.transpose(1, 3, 0, 2).reshape(tokens, D)

    places = jnp.arange(length)
    cosine, sine = angles(places)
    pick_cosine, pick_sine = angles(chosen_places)
    allowed = seen(places, segments, segments)
    pick_segments = jnp.sum(
        jnp.where(chosen_places[:, None] == places[None, :], segments[None, :], 0), axis=1
    )
    pick_allowed = seen(chosen_places, pick_segments, segments)

    start = gather_rows(start_own, "seq").astype(jnp.float32)
    base = params[:13]
    qkv_b, up_b = biases(0)
    qkv_w, out_w, up_w, down_w = weights[0]
    unit0, scale0 = normalized(start)
    first0 = (unit0 * base[0] + base[1]).astype(LOW)
    second0 = (unit0 * base[2] + base[3]).astype(LOW)
    raw = (dot_plain(first0, qkv_w) + qkv_b).reshape(length, 3, heads, HEAD_DIM)
    query0 = rotate(raw[:, 0], cosine, sine).astype(LOW)
    key0 = rotate(raw[:, 1], cosine, sine).astype(LOW)
    value0 = raw[:, 2].astype(LOW)
    mixed0, logsum0 = attend_forward(query0, key0, value0, allowed)
    mixed0 = mixed0.reshape(length, width)
    hidden0 = dot_plain(second0, up_w) + up_b
    active0 = gelu(hidden0).astype(LOW)
    partial = dot_plain(mixed0, out_w) + dot_plain(active0, down_w)
    stream = start_own.astype(jnp.float32) + scatter_sum(partial, "seq") + base[7] + base[12]

    base = params[13:26]
    qkv_b, up_b = biases(1)
    qkv_w, out_w, up_w, down_w = weights[1]
    unit1, scale1 = normalized(stream)
    first_own = (unit1 * base[0] + base[1]).astype(LOW)
    stream_pick = jnp.take(stream, chosen_rows, axis=0)
    unit_pick, scale_pick = normalized(stream_pick)
    first_pick = (unit_pick * base[0] + base[1]).astype(LOW)
    second_pick = (unit_pick * base[2] + base[3]).astype(LOW)
    first1 = gather_rows(first_own, "seq")
    pair = gather_rows(jnp.stack([first_pick, second_pick], axis=1), "seq")
    first1_pick, second1 = pair[:, 0], pair[:, 1]
    raw_q = (dot_plain(first1_pick, qkv_w[:, :width]) + qkv_b[:width]).reshape(-1, heads, HEAD_DIM)
    raw_kv = (dot_plain(first1, qkv_w[:, width:]) + qkv_b[width:]).reshape(length, 2, heads, HEAD_DIM)
    query1 = rotate(raw_q, pick_cosine, pick_sine).astype(LOW)
    key1 = rotate(raw_kv[:, 0], cosine, sine).astype(LOW)
    value1 = raw_kv[:, 1].astype(LOW)
    mixed1, logsum1 = attend_forward(query1, key1, value1, pick_allowed)
    mixed1 = mixed1.reshape(-1, width)
    hidden1 = dot_plain(second1, up_w) + up_b
    active1 = gelu(hidden1).astype(LOW)
    partial = dot_plain(mixed1, out_w) + dot_plain(active1, down_w)
    final_in = stream_pick + scatter_sum(partial, "seq") + base[7] + base[12]

    final_gain, final_shift = params[13 * LAYERS], params[13 * LAYERS + 1]
    unit_f, scale_f = normalized(final_in)
    chosen = (unit_f * final_gain + final_shift).astype(LOW)
    all_rows = gather_chosen(chosen).reshape(-1, D)
    vocab_rows = unembedding.shape[0]
    row_count = all_rows.shape[0]
    goal = all_targets.reshape(groups, members // 2, 2, picks).transpose(2, 0, 1, 3).reshape(-1)
    vocab_start = fsdp_index * vocab_rows
    logits, top, total = score(all_rows, unembedding)
    stats = jnp.concatenate([top, total]).reshape(-1, LANES)
    (stats,) = exchange([stats], [True], ("fsdp",), 2, "gather_stats")
    stats = stats.reshape(members, 2, row_count)
    best = jnp.max(stats[:, 0], axis=0)
    summed = jnp.sum(stats[:, 1] * jnp.exp(stats[:, 0] - best[None]), axis=0)
    logsumexp = best + jnp.log(summed)
    grad_table, own_rows, table_squares, hit = table_grad(
        all_rows, unembedding, logits, goal, logsumexp, vocab_start, seq_index, members // 2 * picks
    )
    grad_chosen = return_chosen(own_rows.reshape(2, members // 2, picks, D))

    grad_gain = jnp.sum(grad_chosen * unit_f, axis=0)
    grad_shift = jnp.sum(grad_chosen, axis=0)
    grad_final = norm_back(unit_f, scale_f, grad_chosen * final_gain)
    low_own = grad_final.astype(LOW)
    bias1 = jnp.sum(low_own.astype(jnp.float32), axis=0)
    grad_low = gather_rows(low_own, "seq")
    grad_active = dot_right(grad_low, down_w)
    _, pull = jax.vjp(gelu, hidden1)
    grad_hidden = pull(grad_active)[0].astype(LOW)
    grad_mixed = dot_right(grad_low, out_w).astype(LOW).reshape(-1, heads, HEAD_DIM)
    grad_q, grad_k, grad_v = attend_backward(query1, key1, value1, pick_allowed, logsum1, grad_mixed)
    raw_gq = rotate_back(grad_q.astype(jnp.float32), pick_cosine, pick_sine).astype(LOW)
    raw_gk = rotate_back(grad_k.astype(jnp.float32), cosine, sine).astype(LOW)
    raw_gq = raw_gq.reshape(-1, width)
    spread_hot = (places[:, None] == chosen_places[None, :]).astype(LOW)
    full_gq = dot_plain(spread_hot, raw_gq).astype(LOW)
    raw_grad1 = jnp.concatenate(
        [full_gq, raw_gk.reshape(length, width), grad_v.reshape(length, width)], axis=1
    )
    part_qkv1 = dot_left(first1, raw_grad1)
    part_out1 = dot_left(mixed1, grad_low)
    part_up1 = dot_left(second1, grad_hidden)
    part_down1 = dot_left(active1, grad_low)
    qkv_bias1 = jnp.sum(raw_grad1.astype(jnp.float32), axis=0)
    up_bias1 = jnp.sum(grad_hidden.astype(jnp.float32), axis=0)
    grad_second = scatter_sum(dot_right(grad_hidden, up_w), "seq")
    grad_first = scatter_sum(dot_right(raw_grad1, qkv_w), "seq")
    gain_rows1 = [
        jnp.sum(grad_first * unit1, axis=0),
        jnp.sum(grad_first, axis=0),
        jnp.sum(grad_second * unit_pick, axis=0),
        jnp.sum(grad_second, axis=0),
    ]
    back_pick = norm_back(unit_pick, scale_pick, grad_second * base[2]) + grad_final
    grad_stream = norm_back(unit1, scale1, grad_first * base[0])
    grad_stream = grad_stream.at[chosen_rows].add(back_pick)

    base = params[:13]
    qkv_w, out_w, up_w, down_w = weights[0]
    low_own = grad_stream.astype(LOW)
    bias0 = jnp.sum(low_own.astype(jnp.float32), axis=0)
    grad_low = gather_rows(low_own, "seq")
    grad_active = dot_right(grad_low, down_w)
    _, pull = jax.vjp(gelu, hidden0)
    grad_hidden = pull(grad_active)[0].astype(LOW)
    grad_mixed = dot_right(grad_low, out_w).astype(LOW).reshape(length, heads, HEAD_DIM)
    grad_q, grad_k, grad_v = attend_backward(query0, key0, value0, allowed, logsum0, grad_mixed)
    raw_gq = rotate_back(grad_q.astype(jnp.float32), cosine, sine).astype(LOW)
    raw_gk = rotate_back(grad_k.astype(jnp.float32), cosine, sine).astype(LOW)
    raw_grad0 = jnp.stack([raw_gq, raw_gk, grad_v], axis=1).reshape(length, 3 * width)
    part_qkv0 = dot_left(first0, raw_grad0)
    part_out0 = dot_left(mixed0, grad_low)
    part_up0 = dot_left(second0, grad_hidden)
    part_down0 = dot_left(active0, grad_low)
    qkv_bias0 = jnp.sum(raw_grad0.astype(jnp.float32), axis=0)
    up_bias0 = jnp.sum(grad_hidden.astype(jnp.float32), axis=0)
    grad_first = dot_right(raw_grad0, qkv_w)
    grad_second = dot_right(grad_hidden, up_w)
    gain_rows0 = [
        jnp.sum(grad_first * unit0, axis=0),
        jnp.sum(grad_first, axis=0),
        jnp.sum(grad_second * unit0, axis=0),
        jnp.sum(grad_second, axis=0),
    ]
    own = seq_index * tokens
    grad_unit = scatter_sum(grad_first * base[0] + grad_second * base[2], "seq")
    grad_stream = grad_stream + norm_back(
        lax.dynamic_slice_in_dim(unit0, own, tokens, 0),
        lax.dynamic_slice_in_dim(scale0, own, tokens, 0),
        grad_unit,
    )

    def to_owner(part_qkv, part_out, part_up, part_down):
        def by_owner(value):
            value = value.reshape(groups, members, local, value.shape[1])
            return value.transpose(1, 0, 2, 3).reshape(members, groups * local, value.shape[3])

        block = jnp.concatenate(
            [
                by_owner(part_up),
                part_down.reshape(members, inner, D),
                part_out.reshape(members, local, D),
            ],
            axis=1,
        )
        block = lax.psum_scatter(block.reshape(-1, D), "fsdp", scatter_dimension=0, tiled=True)
        qkv = lax.psum_scatter(
            by_owner(part_qkv).reshape(-1, 3 * width), "fsdp", scatter_dimension=0, tiled=True
        )
        up = block[: groups * local].reshape(groups, local, hidden)
        down = block[groups * local : groups * local + inner]
        out = block[groups * local + inner :]
        return qkv.reshape(groups, local, 3 * width), out, up, down

    parts1 = to_owner(part_qkv1, part_out1, part_up1, part_down1)
    parts0 = to_owner(part_qkv0, part_out0, part_up0, part_down0)
    moved = exchange(
        [parts0[0], parts1[0], parts0[2], parts1[2]], [False] * 4, ("seq",), 6, "part_grads"
    )

    def owned(depth):
        qkv = moved[depth].reshape(groups, local, 3, width)
        qkv = qkv.transpose(1, 2, 0, 3).reshape(local, 3 * D)
        up = moved[LAYERS + depth].transpose(1, 0, 2).reshape(local, groups * hidden)
        other = (parts0, parts1)[depth]
        return qkv, other[1], up, other[3]

    layer_grads = [owned(depth) for depth in range(LAYERS)]

    def whole(vector, size, count):
        spot = jnp.zeros((count, groups, size), jnp.float32)
        spot = lax.dynamic_update_slice(spot, vector.reshape(count, 1, size), (0, seq_index, 0))
        return spot.reshape(count, groups * size)

    def vector_rows(gain_rows, qkv_bias, up_bias, bias):
        return jnp.concatenate(
            [
                jnp.stack(gain_rows),
                whole(qkv_bias, width, 3),
                bias[None],
                whole(up_bias, hidden, 1).reshape(-1, D),
                bias[None],
            ]
        )

    vector_grad = jnp.concatenate(
        [
            vector_rows(gain_rows0, qkv_bias0, up_bias0, bias0),
            vector_rows(gain_rows1, qkv_bias1, up_bias1, bias1),
            jnp.stack([grad_gain, grad_shift]),
        ]
    )
    vector_send = vector_grad.reshape(rows, groups * members, columns).transpose(1, 0, 2)
    vector_send = vector_send.reshape(groups * members, rows * columns)
    spare = -(rows * columns) % 1024
    vector_send = jnp.pad(vector_send, ((0, 0), (0, spare))).reshape(groups * members, -1, 128)
    row_send = grad_stream.astype(LOW).reshape(chunks, LANES, groups * members, columns)
    row_send = row_send.transpose(2, 0, 3, 1)
    row_back, vector_back = exchange(
        [row_send, vector_send], [False, False], BOTH, 3, "return_rows"
    )
    grad_vectors = jnp.sum(vector_back, axis=0).reshape(-1)[: rows * columns].reshape(rows, columns)
    vocab = embedding.shape[0]
    grad_embedding, embedding_squares = add_rows(
        all_ids, row_back.reshape(-1, columns, LANES), vocab
    )
    grad_embedding = grad_embedding[:, :vocab].T

    grads = (
        grad_embedding,
        grad_table,
        jnp.stack([layer_grads[depth][0] for depth in range(LAYERS)]),
        jnp.stack([layer_grads[depth][1] for depth in range(LAYERS)]),
        jnp.stack([layer_grads[depth][2] for depth in range(LAYERS)]),
        jnp.stack([layer_grads[depth][3] for depth in range(LAYERS)]),
        grad_vectors,
    )
    squares = jnp.sum(embedding_squares)
    squares = squares + jnp.where(seq_index == 0, jnp.sum(table_squares), 0.0)
    for grad in grads[2:]:
        squares = squares + jnp.sum(grad * grad)
    hits = jnp.where(seq_index == 0, jnp.sum(hit), 0.0)
    place = lax.broadcasted_iota(jnp.int32, (8, LANES), 0)
    (norm_parts,) = exchange(
        [jnp.where(place == 0, squares, hits)], [True], BOTH, 4, "gather_norm"
    )
    totals = jnp.sum(norm_parts[:, :2, 0], axis=0)
    grad_norm = jnp.sqrt(totals[0])
    loss = (jnp.sum(logsumexp) - totals[1]) / row_count
    factor = jnp.minimum(1.0, clip_limit / grad_norm)
    weights_all = (
        embedding,
        unembedding,
        query_key_value_weight,
        attention_output_weight,
        up_projection,
        down_projection,
        vectors,
    )
    means = (
        embedding_mean,
        unembedding_mean,
        input_proj_mean,
        output_proj_mean,
        up_proj_mean,
        down_proj_mean,
        vectors_mean,
    )
    seconds = (
        embedding_square,
        unembedding_square,
        input_proj_square,
        output_proj_square,
        up_proj_square,
        down_proj_square,
        vectors_square,
    )
    result = [
        adamw(weights_all[index], means[index], seconds[index], grads[index], factor)
        for index in range(7)
    ]
    return (loss, grad_norm) + tuple(result[index][kind] for kind in range(3) for index in range(7))


def solution(mesh):
    state = (
        P(None, BOTH),
        P("fsdp", None),
        P(None, BOTH, None),
        P(None, BOTH, None),
        P(None, BOTH, None),
        P(None, BOTH, None),
        P(None, BOTH),
    )
    in_specs = (P("fsdp", "seq"),) * 3 + state * 3
    out_specs = (P(), P()) + state * 3
    return jax.shard_map(body, mesh=mesh, in_specs=in_specs, out_specs=out_specs, check_vma=False)
```
